1024 devices in a mesh: lat: 16 (over x_lo, y, core), lon: 64 (over z, x_hi).
Axes of the slice: x: 4 (x_hi: 2, x_lo: 2; x = x_hi * 2 + x_lo), y: 4, z: 32, core: 2. Of those that a mesh axis runs over, the one named last changes fastest.
Arguments:
- tracers: bfloat16 [10, 4, 256, 8192], P(None, None, 'lat', 'lon'), may hold values from -6 to 6
- winds: float32 [3, 4, 256, 8192], P(None, None, 'lat', 'lon'), may hold values from -2.5 to 2.5
- zonal_shift: int32 [256], P('lat'), may hold values from 0 to 8191
Outputs:
- new_tracers: bfloat16 [10, 4, 256, 8192], P(None, None, 'lat', 'lon')
- displacement: float32 [3, 4, 256, 8192], P(None, None, 'lat', 'lon')
The draws below stay inside these ranges and needn't reach their ends.
All inputs are finite; a program needn't handle non-finite values.
Results may differ from the reference program's by a relative error of at most 0.001.
Values may be sent and summed in bfloat16 or wider, within the bound.
No kernel may reach another device: no remote copies, remote signals or barrier semaphores. Data moves between devices by JAX's collectives and lax.ppermute only.
A program may use at most 64 MiB of HBM per device.

```python
import jax
import jax.numpy as jnp
from jax import lax

NTR = 10
LEV = 4
ITERS = 3
NLAT = 256
NLON = 8192


def plant(drawn, own_key, least, largest):
    index_at = [jax.random.randint(jax.random.fold_in(own_key, axis), (), 0, length) for axis, length in enumerate(drawn.shape)]
    longest = drawn.shape.index(max(drawn.shape))
    beside = index_at[:longest] + [(index_at[longest] + 1) % drawn.shape[longest]] + index_at[longest + 1:]
    return drawn.at[tuple(index_at)].set(least).at[tuple(beside)].set(largest)


def steps_of(own_key, extent, pieces, least, high):
    def one(position, shards_of):
        heights = jax.random.uniform(jax.random.fold_in(jax.random.fold_in(own_key, 6), position), (shards_of,), jnp.float32, least / len(pieces), high / len(pieces))
        return jnp.repeat(jnp.exp(heights), extent[position] // shards_of).reshape((-1,) + (1,) * (len(extent) - position - 1))

    factor_of = one(*pieces[0])
    for cut in pieces[1:]:
        factor_of = factor_of * one(*cut)
    return factor_of


def gaussian(rng, extent, spread, limit, split=(), held_as=jnp.bfloat16):
    drawn = jax.random.normal(rng, extent, jnp.float32) * spread
    if len(split) > 0:
        drawn = steps_of(rng, extent, split, -0.22, 0.18) * drawn
    return jnp.clip(drawn, min=-limit, max=limit).astype(held_as)


def setup_inputs(seed: int = 0) -> dict:
    key_of = jax.random.split(jax.random.key(seed), 4)
    tracers = gaussian(key_of[0], (NTR, LEV, NLAT, NLON), 1.0, 6.0, ((2, 16), (3, 64)))
    winds = jnp.clip(jax.random.uniform(key_of[1], (3, LEV, NLAT, NLON), jnp.float32, -2.5, 2.5) * steps_of(key_of[1], (3, LEV, NLAT, NLON), ((2, 16), (3, 64)), -0.4, 0.0), -2.5, 2.5)
    zonal_shift = plant(jax.random.randint(key_of[2], (NLAT,), 0, NLON), jax.random.fold_in(key_of[2], 1), 0, NLON - 1).astype(jnp.int32)
    return dict(tracers=tracers, winds=winds, zonal_shift=zonal_shift)


def cubic_weights(frac):
    return (-frac * (frac - 1.0) * (frac - 2.0) / 6.0,
            (frac + 1.0) * (frac - 1.0) * (frac - 2.0) / 2.0,
            -(frac + 1.0) * frac * (frac - 2.0) / 2.0,
            (frac + 1.0) * frac * (frac - 1.0) / 6.0)


def reference(tracers, winds, zonal_shift):
    shape = (LEV, NLAT, NLON)
    kpos = lax.broadcasted_iota(jnp.float32, shape, 0)
    gpos = lax.broadcasted_iota(jnp.float32, shape, 1)
    jcol = lax.broadcasted_iota(jnp.int32, shape, 2)
    wide = jnp.pad(winds, ((0, 0), (1, 1), (2, 2), (0, 0))).reshape(3, -1)

    def wind_at(disp):
        zlev = jnp.clip(kpos - 0.5 * disp[0], 0.0, LEV - 1.0)
        ylat = jnp.clip(gpos - 0.5 * disp[1], 0.0, NLAT - 1.0)
        xrel = -0.5 * disp[2]
        zb = jnp.floor(zlev)
        yb = jnp.floor(ylat)
        xb = jnp.floor(xrel)
        tz = zlev - zb
        ty = ylat - yb
        tx = xrel - xb
        zi = zb.astype(jnp.int32) + 1
        yi = yb.astype(jnp.int32) + 2
        xi = jcol + xb.astype(jnp.int32)
        wz = (1.0 - tz, tz)
        wy = (1.0 - ty, ty)
        wx = (1.0 - tx, tx)
        total = jnp.zeros((3,) + shape, jnp.float32)
        for a in range(2):
            for b in range(2):
                for c in range(2):
                    index = ((zi + a) * (NLAT + 4) + (yi + b)) * NLON + jnp.mod(xi + c, NLON)
                    picked = jnp.take(wide, index.reshape(-1), axis=1).reshape((3,) + shape)
                    total = total + (wz[a] * wy[b] * wx[c]) * picked
        return total

    disp = winds
    for step in range(ITERS):
        disp = wind_at(disp)

    colrow = lax.broadcasted_iota(jnp.int32, (NLAT, NLON), 1)
    source_col = jnp.mod(colrow - zonal_shift[:, None], NLON).astype(jnp.int32)
    source_col = jnp.broadcast_to(source_col[None, None], tracers.shape)
    moved = jnp.take_along_axis(tracers, source_col, axis=3)

    zdep = jnp.clip(kpos - disp[0], 0.0, LEV - 1.0)
    ydep = jnp.clip(gpos - disp[1], 0.0, NLAT - 1.0)
    xrel = -disp[2]
    zb = jnp.floor(zdep)
    yb = jnp.floor(ydep)
    xb = jnp.floor(xrel)
    wz = cubic_weights(zdep - zb)
    wy = cubic_weights(ydep - yb)
    wx = cubic_weights(xrel - xb)
    zi = zb.astype(jnp.int32) + 1
    yi = yb.astype(jnp.int32) + 1
    base_col = jcol + xb.astype(jnp.int32) - 1
    padded = jnp.pad(moved, ((0, 0), (2, 2), (2, 2), (0, 0))).reshape(NTR, -1)
    result = jnp.zeros((NTR,) + shape, jnp.float32)
    for a in range(4):
        for b in range(4):
            partial_value = jnp.zeros((NTR,) + shape, jnp.float32)
            for c in range(4):
                index = ((zi + a) * (NLAT + 4) + (yi + b)) * NLON + jnp.mod(base_col + c, NLON)
                picked = jnp.take(padded, index.reshape(-1), axis=1).reshape((NTR,) + shape)
                partial_value = partial_value + wx[c] * picked
            result = result + (wz[a] * wy[b]) * partial_value
    return result.astype(jnp.bfloat16), disp
```

```python
import jax
import jax.numpy as jnp
from jax import lax
from jax.experimental import pallas as pl
from jax.experimental.pallas import tpu as pltpu
from jax.sharding import PartitionSpec as P


ITERS = 3
RIM = 4
LANES = 128
SPAN = 9


def ring_shift(x, axis, by):
    length = lax.axis_size(axis)
    return lax.ppermute(x, axis, [(i, (i + by) % length) for i in range(length)])


def padded(block, sides, width):
    for axis, dim in sides:
        low = ring_shift(lax.slice_in_dim(block, block.shape[dim] - width, None, axis=dim), axis, 1)
        high = ring_shift(lax.slice_in_dim(block, 0, width, axis=dim), axis, -1)
        block = jnp.concatenate([low, block, high], axis=dim)
    return block


def cubic_weights(frac):
    return (
        -frac * (frac - 1.0) * (frac - 2.0) / 6.0,
        (frac + 1.0) * (frac - 1.0) * (frac - 2.0) / 2.0,
        -(frac + 1.0) * frac * (frac - 2.0) / 2.0,
        (frac + 1.0) * frac * (frac - 1.0) / 6.0,
    )


def spread(base, weights, lowest, highest):
    listed = []
    for target in range(lowest, highest + 1):
        summed = jnp.zeros(base.shape, jnp.float32)
        for a in range(len(weights)):
            summed = summed + jnp.where(base + a == target, weights[a], 0.0)
        listed.append(summed)
    return listed


def pole_zero(block, width, anchor, total_rows):
    rowpos = lax.broadcasted_iota(jnp.int32, (block.shape[2], 1), 0) + anchor - width
    keep = (rowpos >= 0) & (rowpos < total_rows)
    return jnp.where(keep, block, jnp.zeros_like(block))


def trajectory(winds, anchor, total_rows):
    _, levels, rows, cols = winds.shape
    shape = (levels, rows, cols)
    kpos = lax.broadcasted_iota(jnp.float32, shape, 0)
    kint = lax.broadcasted_iota(jnp.int32, shape, 0)
    growi = lax.broadcasted_iota(jnp.int32, shape, 1) + anchor
    gpos = growi.astype(jnp.float32)
    wide = padded(winds, (("lon", 3), ("lat", 2)), 2)
    wide = pole_zero(wide, 2, anchor, total_rows)
    wide = jnp.pad(wide, ((0, 0), (2, 2), (0, 0), (0, 0)))
    disp = winds
    for _ in range(ITERS):
        zlev = jnp.clip(kpos - 0.5 * disp[0], 0.0, levels - 1.0)
        ylat = jnp.clip(gpos - 0.5 * disp[1], 0.0, total_rows - 1.0)
        xrel = -0.5 * disp[2]
        zb = jnp.floor(zlev)
        yb = jnp.floor(ylat)
        xb = jnp.floor(xrel)
        tz = zlev - zb
        ty = ylat - yb
        tx = xrel - xb
        z_weights = spread(zb.astype(jnp.int32) - kint, (1.0 - tz, tz), -2, 2)
        y_weights = spread(yb.astype(jnp.int32) - growi, (1.0 - ty, ty), -2, 2)
        x_weights = spread(xb.astype(jnp.int32), (1.0 - tx, tx), -2, 2)
        total = jnp.zeros((3,) + shape, jnp.float32)
        for iz in range(5):
            plane = jnp.zeros((3,) + shape, jnp.float32)
            for iy in range(5):
                line = jnp.zeros((3,) + shape, jnp.float32)
                for ix in range(5):
                    line = line + x_weights[ix] * wide[:, iz : iz + levels, iy : iy + rows, ix : ix + cols]
                plane = plane + y_weights[iy] * line
            total = total + z_weights[iz] * plane
        disp = total
    return disp


def lane_pick(x, index):
    return jnp.take_along_axis(x, index, axis=1)


def iota2(dim):
    return lax.broadcasted_iota(jnp.int32, (8, LANES), dim)


def prepare(tracers, shifts, westward, sectors):
    ntrac, levels, rows, cols = tracers.shape
    height = ntrac * rows + 16

    def body(west_ref, shift_ref, in_ref, out_ref, hop_ref, rim_ref):
        lane = iota2(1)
        sub = iota2(0)
        picks, hops, places = [], [], []
        edge = jnp.where((lane & 7) < RIM, cols - RIM + (lane & 7), (lane & 7) - RIM)
        step = jnp.where((lane & 7) < RIM, 1, -1)
        rim_hops = jnp.zeros((1, LANES), jnp.float32)
        for g in range(rows // 8):
            total = shift_ref[8 * g : 8 * g + 8, :]
            within = total & (cols - 1)
            picks.append((lane - within) & (cols - 1))
            hop = (total >> 7) + jnp.where(lane < within, 1, 0)
            hops.append(hop)
            places.append((lane >> 3) == sub + 8 * g)
            edge_hop = lane_pick(hop.astype(jnp.float32), edge)
            rim_hops = rim_hops + jnp.sum(jnp.where(places[g], edge_hop, 0.0), axis=0, keepdims=True)
        rim_hop = jnp.broadcast_to(rim_hops, (8, LANES)).astype(jnp.int32) + step
        hops = [jnp.where(west_ref[0] == 1, -hop, hop) & (sectors - 1) for hop in hops + [rim_hop]]
        for t in range(ntrac):
            for g in range(rows // 8):
                hop_ref[t * rows + 8 * g : t * rows + 8 * g + 8, :] = hops[g]
        hop_ref[height - 16 : height - 8, :] = hops[-1]
        hop_ref[height - 8 : height, :] = hops[-1]
        rim_ref[...] = jnp.zeros_like(rim_ref)

        def level(k, carry):
            for t in range(ntrac):
                block = in_ref[t, k].astype(jnp.float32)
                turned = []
                rim = jnp.zeros((8, LANES), jnp.float32)
                for g in range(rows // 8):
                    part = lane_pick(block[8 * g : 8 * g + 8], picks[g])
                    turned.append(part)
                    rim = rim + jnp.where(places[g], lane_pick(part, edge), 0.0)
                out_ref[k, t * rows : (t + 1) * rows, :] = jnp.concatenate(turned, axis=0).astype(jnp.bfloat16)
                rim_ref[t : t + 1, :] = jnp.sum(rim, axis=0, keepdims=True)
            out_ref[k, height - 16 : height, :] = rim_ref[...].astype(jnp.bfloat16)
            return carry

        lax.fori_loop(0, levels, level, 0)

    smem = pl.BlockSpec(memory_space=pltpu.SMEM)
    vmem = pl.BlockSpec(memory_space=pltpu.VMEM)
    return pl.pallas_call(
        body,
        out_shape=(
            jax.ShapeDtypeStruct((levels, height, LANES), jnp.bfloat16),
            jax.ShapeDtypeStruct((height, LANES), jnp.int32),
        ),
        in_specs=[smem, vmem, vmem],
        scratch_shapes=[pltpu.VMEM((16, LANES), jnp.float32)],
        name="prepare",
    )(westward, shifts, tracers)


def edges_of(main, ntrac, rows):
    levels, height, _ = main.shape
    cut = -(-ntrac * RIM // 8) * 8

    def body(main_ref, first_ref, last_ref, a_ref, b_ref):
        a_ref[...] = jnp.zeros_like(a_ref)
        b_ref[...] = jnp.zeros_like(b_ref)
        for k in range(levels):
            for t in range(ntrac):
                block = main_ref[k, t * rows : (t + 1) * rows, :].astype(jnp.float32)
                a_ref[t * RIM : (t + 1) * RIM, :] = block[:RIM]
                b_ref[t * RIM : (t + 1) * RIM, :] = block[rows - RIM :]
            rim = main_ref[k, height - 16 : height, :]
            first_ref[k, :cut, :] = a_ref[...].astype(jnp.bfloat16)
            last_ref[k, :cut, :] = b_ref[...].astype(jnp.bfloat16)
            first_ref[k, cut:, :] = rim
            last_ref[k, cut:, :] = rim

    edge = jax.ShapeDtypeStruct((levels, cut + 16, LANES), jnp.bfloat16)
    return pl.pallas_call(
        body,
        out_shape=(edge, edge),
        scratch_shapes=[pltpu.VMEM((cut, LANES), jnp.float32), pltpu.VMEM((cut, LANES), jnp.float32)],
        name="edges_of",
    )(main)


def interpolate(place, disp, main, below, above, ntrac, rows, total_rows):
    levels = main.shape[0]
    height = ntrac * rows + 16
    groups = rows // 8
    tall = rows + 2 * RIM
    weight_count = 2 * SPAN + levels
    cut = ntrac * RIM

    def body(
        place_ref, disp_ref, main_ref, below_ref, above_ref, out_ref, weight_ref, rim_ref, end_ref, even_ref, odd_ref
    ):
        lane = iota2(1)
        sub = iota2(0)
        anchor = place_ref[0]
        has_below = place_ref[0] > 0
        has_above = place_ref[0] + rows < total_rows

        def weigh(k, carry):
            for g in range(groups):
                at = pl.ds(8 * g, 8)
                row_index = sub + (8 * g) + anchor
                zdep = jnp.clip(k.astype(jnp.float32) - disp_ref[0, k, at, :], 0.0, levels - 1.0)
                ydep = jnp.clip(row_index.astype(jnp.float32) - disp_ref[1, k, at, :], 0.0, total_rows - 1.0)
                xrel = -disp_ref[2, k, at, :]
                zb = jnp.floor(zdep)
                yb = jnp.floor(ydep)
                xb = jnp.floor(xrel)
                x_weights = spread(xb.astype(jnp.int32) - 1, cubic_weights(xrel - xb), -4, 4)
                y_weights = spread(yb.astype(jnp.int32) - row_index - 1, cubic_weights(ydep - yb), -4, 4)
                z_weights = spread(zb.astype(jnp.int32) - 1, cubic_weights(zdep - zb), 0, levels - 1)
                for n, value in enumerate(x_weights + y_weights + z_weights):
                    weight_ref[(k * groups + g) * weight_count + n] = value
            return carry

        lax.fori_loop(0, levels, weigh, 0)

        for l in range(levels):
            rim_ref[l, 0] = main_ref[l, height - 16 : height, :].astype(jnp.float32)
            rim_ref[l, 1] = jnp.where(has_below, below_ref[l, cut:, :].astype(jnp.float32), 0.0)
            rim_ref[l, 2] = jnp.where(has_above, above_ref[l, cut:, :].astype(jnp.float32), 0.0)
            end_ref[l, 0] = jnp.where(has_below, below_ref[l, :cut, :].astype(jnp.float32), 0.0)
            end_ref[l, 1] = jnp.where(has_above, above_ref[l, :cut, :].astype(jnp.float32), 0.0)

        near = (lane + RIM) & 7

        def build(t, to_ref):
            base = pl.multiple_of(t * rows, rows)
            for l in range(levels):
                own = jnp.broadcast_to(rim_ref[l, 0, pl.ds(t, 1), :], (8, LANES))
                block = main_ref[l, pl.ds(base, rows), :].astype(jnp.float32)
                ends = [end_ref[l, n, pl.ds(t * RIM, RIM), :] for n in range(2)]
                block = jnp.concatenate([ends[0], block, ends[1]], axis=0)
                lower = jnp.broadcast_to(rim_ref[l, 1, pl.ds(t, 1), :], (8, LANES))
                upper = jnp.broadcast_to(rim_ref[l, 2, pl.ds(t, 1), :], (8, LANES))
                for v in range(tall // 8):
                    inner_row = sub + (8 * v - RIM)
                    source = own
                    if v == 0:
                        source = jnp.where(sub < RIM, lower, own)
                    if v == tall // 8 - 1:
                        source = jnp.where(sub >= RIM, upper, own)
                    edges = lane_pick(source, ((inner_row & (rows - 1)) << 3) + near)
                    middle = block[8 * v : 8 * v + 8]
                    for ix in range(SPAN):
                        o = ix - RIM
                        if o > 0:
                            value = pltpu.roll(jnp.where(lane < o, edges, middle), LANES - o, 1)
                        elif o < 0:
                            value = pltpu.roll(jnp.where(lane >= LANES + o, edges, middle), -o, 1)
                        else:
                            value = middle
                        to_ref[l * SPAN + ix, 8 * v : 8 * v + 8, :] = value

        def cells(t, kp, from_ref):
            results = [[], []]
            for g in range(groups):
                at = [((2 * kp + h) * groups + g) * weight_count for h in range(2)]
                wx = [[weight_ref[at[h] + n] for n in range(SPAN)] for h in range(2)]
                result = [None, None]
                for l in range(levels):
                    plane = [None, None]
                    for iy in range(SPAN):
                        line = [None, None]
                        first = 8 * g + iy
                        for ix in range(SPAN):
                            value = from_ref[l * SPAN + ix, first : first + 8, :]
                            for h in range(2):
                                term = wx[h][ix] * value
                                line[h] = term if ix == 0 else line[h] + term
                        for h in range(2):
                            term = weight_ref[at[h] + SPAN + iy] * line[h]
                            plane[h] = term if plane[h] is None else plane[h] + term
                    for h in range(2):
                        term = weight_ref[at[h] + 2 * SPAN + l] * plane[h]
                        result[h] = term if l == 0 else result[h] + term
                for h in range(2):
                    results[h].append(result[h])
            for h in range(2):
                out_ref[t, 2 * kp + h] = jnp.concatenate(results[h], axis=0).astype(jnp.bfloat16)

        build(0, even_ref)

        def tracers(pair, carry):
            t = 2 * pair
            build(t + 1, odd_ref)
            for kp in range(levels // 2):
                cells(t, kp, even_ref)
            build(jnp.minimum(t + 2, ntrac - 1), even_ref)
            for kp in range(levels // 2):
                cells(t + 1, kp, odd_ref)
            return carry

        lax.fori_loop(0, ntrac // 2, tracers, 0)

    smem = pl.BlockSpec(memory_space=pltpu.SMEM)
    vmem = pl.BlockSpec(memory_space=pltpu.VMEM)
    return pl.pallas_call(
        body,
        out_shape=jax.ShapeDtypeStruct((ntrac, levels, rows, LANES), jnp.bfloat16),
        in_specs=[smem] + [vmem] * 4,
        scratch_shapes=[
            pltpu.VMEM((levels * groups * weight_count, 8, LANES), jnp.float32),
            pltpu.VMEM((levels, 3, 16, LANES), jnp.float32),
            pltpu.VMEM((levels, 2, cut, LANES), jnp.float32),
            pltpu.VMEM((levels * SPAN, tall, LANES), jnp.float32),
            pltpu.VMEM((levels * SPAN, tall, LANES), jnp.float32),
        ],
        name="interpolate",
    )(place, disp, main, below, above)


def parity_shift(x, by):
    tall = lax.axis_size("lat")
    wide = lax.axis_size("lon")
    pairs = []
    for a in range(tall):
        way = -by if a & 1 else by
        pairs += [(a * wide + b, a * wide + (b + way) % wide) for b in range(wide)]
    return lax.ppermute(x, ("lat", "lon"), pairs)


def local(tracers, winds, zonal_shift):
    ntrac, _, rows, _ = tracers.shape
    sectors = lax.axis_size("lon")
    total_rows = rows * lax.axis_size("lat")
    anchor = lax.axis_index("lat") * rows
    place = anchor.reshape(1)
    shifts = jnp.broadcast_to(zonal_shift[:, None], (rows, LANES))
    odd = lax.axis_index("lat") & 1
    main, hops = prepare(tracers, shifts, odd.reshape(1), sectors)
    for bit in range(sectors.bit_length() - 1):
        moved = parity_shift(main, 1 << bit)
        main = jnp.where((hops >> bit & 1) == 1, moved, main)
    disp = trajectory(winds, anchor, total_rows)
    first, last = edges_of(main, ntrac, rows)
    below = ring_shift(last, "lat", 1)
    above = ring_shift(first, "lat", -1)
    new = interpolate(place, disp, main, below, above, ntrac, rows, total_rows)
    return new, disp


def solution(mesh):
    return jax.shard_map(
        local,
        mesh=mesh,
        in_specs=(P(None, None, "lat", "lon"), P(None, None, "lat", "lon"), P("lat")),
        out_specs=(P(None, None, "lat", "lon"), P(None, None, "lat", "lon")),
        check_vma=False,
    )
```

```python
import jax
import jax.numpy as jnp
from jax import lax
from jax.experimental import pallas as pl
from jax.experimental.pallas import tpu as pltpu
from jax.sharding import PartitionSpec as P


ITERS = 3
RIM = 4
LANES = 128
SPAN = 9


def ring_shift(x, axis, by):
    length = lax.axis_size(axis)
    return lax.ppermute(x, axis, [(i, (i + by) % length) for i in range(length)])


def padded(block, sides, width):
    for axis, dim in sides:
        low = ring_shift(lax.slice_in_dim(block, block.shape[dim] - width, None, axis=dim), axis, 1)
        high = ring_shift(lax.slice_in_dim(block, 0, width, axis=dim), axis, -1)
        block = jnp.concatenate([low, block, high], axis=dim)
    return block


def cubic_weights(frac):
    return (
        -frac * (frac - 1.0) * (frac - 2.0) / 6.0,
        (frac + 1.0) * (frac - 1.0) * (frac - 2.0) / 2.0,
        -(frac + 1.0) * frac * (frac - 2.0) / 2.0,
        (frac + 1.0) * frac * (frac - 1.0) / 6.0,
    )


def spread(base, weights, lowest, highest):
    listed = []
    for target in range(lowest, highest + 1):
        summed = jnp.zeros(base.shape, jnp.float32)
        for a in range(len(weights)):
            summed = summed + jnp.where(base + a == target, weights[a], 0.0)
        listed.append(summed)
    return listed


def pole_zero(block, width, anchor, total_rows):
    rowpos = lax.broadcasted_iota(jnp.int32, (block.shape[2], 1), 0) + anchor - width
    keep = (rowpos >= 0) & (rowpos < total_rows)
    return jnp.where(keep, block, jnp.zeros_like(block))


def trajectory(winds, anchor, total_rows):
    _, levels, rows, cols = winds.shape
    shape = (levels, rows, cols)
    kpos = lax.broadcasted_iota(jnp.float32, shape, 0)
    kint = lax.broadcasted_iota(jnp.int32, shape, 0)
    growi = lax.broadcasted_iota(jnp.int32, shape, 1) + anchor
    gpos = growi.astype(jnp.float32)
    wide = padded(winds, (("lon", 3), ("lat", 2)), 2)
    wide = pole_zero(wide, 2, anchor, total_rows)
    wide = jnp.pad(wide, ((0, 0), (2, 2), (0, 0), (0, 0)))
    disp = winds
    for _ in range(ITERS):
        zlev = jnp.clip(kpos - 0.5 * disp[0], 0.0, levels - 1.0)
        ylat = jnp.clip(gpos - 0.5 * disp[1], 0.0, total_rows - 1.0)
        xrel = -0.5 * disp[2]
        zb = jnp.floor(zlev)
        yb = jnp.floor(ylat)
        xb = jnp.floor(xrel)
        tz = zlev - zb
        ty = ylat - yb
        tx = xrel - xb
        z_weights = spread(zb.astype(jnp.int32) - kint, (1.0 - tz, tz), -2, 2)
        y_weights = spread(yb.astype(jnp.int32) - growi, (1.0 - ty, ty), -2, 2)
        x_weights = spread(xb.astype(jnp.int32), (1.0 - tx, tx), -2, 2)
        total = jnp.zeros((3,) + shape, jnp.float32)
        for iz in range(5):
            plane = jnp.zeros((3,) + shape, jnp.float32)
            for iy in range(5):
                line = jnp.zeros((3,) + shape, jnp.float32)
                for ix in range(5):
                    line = line + x_weights[ix] * wide[:, iz : iz + levels, iy : iy + rows, ix : ix + cols]
                plane = plane + y_weights[iy] * line
            total = total + z_weights[iz] * plane
        disp = total
    return disp


def resident(x):
    return pltpu.with_memory_space_constraint(x, pltpu.VMEM)


def lane_pick(x, index):
    return jnp.take_along_axis(x, index, axis=1)


def iota2(dim):
    return lax.broadcasted_iota(jnp.int32, (8, LANES), dim)


def prepare(tracers, shifts, westward, sectors):
    ntrac, levels, rows, cols = tracers.shape
    height = ntrac * rows + 16

    def body(west_ref, shift_ref, in_ref, out_ref, hop_ref, rim_ref):
        lane = iota2(1)
        sub = iota2(0)
        picks, hops, places = [], [], []
        edge = jnp.where((lane & 7) < RIM, cols - RIM + (lane & 7), (lane & 7) - RIM)
        step = jnp.where((lane & 7) < RIM, 1, -1)
        rim_hops = jnp.zeros((1, LANES), jnp.float32)
        for g in range(rows // 8):
            total = shift_ref[8 * g : 8 * g + 8, :]
            within = total & (cols - 1)
            picks.append((lane - within) & (cols - 1))
            hop = (total >> 7) + jnp.where(lane < within, 1, 0)
            hops.append(hop)
            places.append((lane >> 3) == sub + 8 * g)
            edge_hop = lane_pick(hop.astype(jnp.float32), edge)
            rim_hops = rim_hops + jnp.sum(jnp.where(places[g], edge_hop, 0.0), axis=0, keepdims=True)
        rim_hop = jnp.broadcast_to(rim_hops, (8, LANES)).astype(jnp.int32) + step
        hops = [jnp.where(west_ref[0] == 1, -hop, hop) & (sectors - 1) for hop in hops + [rim_hop]]
        for t in range(ntrac):
            for g in range(rows // 8):
                hop_ref[t * rows + 8 * g : t * rows + 8 * g + 8, :] = hops[g]
        hop_ref[height - 16 : height - 8, :] = hops[-1]
        hop_ref[height - 8 : height, :] = hops[-1]
        rim_ref[...] = jnp.zeros_like(rim_ref)

        def level(k, carry):
            for t in range(ntrac):
                block = in_ref[t, k].astype(jnp.float32)
                turned = []
                rim = jnp.zeros((8, LANES), jnp.float32)
                for g in range(rows // 8):
                    part = lane_pick(block[8 * g : 8 * g + 8], picks[g])
                    turned.append(part)
                    rim = rim + jnp.where(places[g], lane_pick(part, edge), 0.0)
                out_ref[k, t * rows : (t + 1) * rows, :] = jnp.concatenate(turned, axis=0).astype(jnp.bfloat16)
                rim_ref[t : t + 1, :] = jnp.sum(rim, axis=0, keepdims=True)
            out_ref[k, height - 16 : height, :] = rim_ref[...].astype(jnp.bfloat16)
            return carry

        lax.fori_loop(0, levels, level, 0)

    smem = pl.BlockSpec(memory_space=pltpu.SMEM)
    vmem = pl.BlockSpec(memory_space=pltpu.VMEM)
    return pl.pallas_call(
        body,
        out_shape=(
            pltpu.VMEM((levels, height, LANES), jnp.bfloat16),
            pltpu.VMEM((height, LANES), jnp.int32),
        ),
        in_specs=[smem, vmem, vmem],
        scratch_shapes=[pltpu.VMEM((16, LANES), jnp.float32)],
        name="prepare",
    )(westward, shifts, tracers)


def edges_of(main, ntrac, rows):
    levels, height, _ = main.shape
    cut = -(-ntrac * RIM // 8) * 8

    def body(main_ref, first_ref, last_ref, a_ref, b_ref):
        a_ref[...] = jnp.zeros_like(a_ref)
        b_ref[...] = jnp.zeros_like(b_ref)
        for k in range(levels):
            for t in range(ntrac):
                block = main_ref[k, t * rows : (t + 1) * rows, :].astype(jnp.float32)
                a_ref[t * RIM : (t + 1) * RIM, :] = block[:RIM]
                b_ref[t * RIM : (t + 1) * RIM, :] = block[rows - RIM :]
            rim = main_ref[k, height - 16 : height, :]
            first_ref[k, :cut, :] = a_ref[...].astype(jnp.bfloat16)
            last_ref[k, :cut, :] = b_ref[...].astype(jnp.bfloat16)
            first_ref[k, cut:, :] = rim
            last_ref[k, cut:, :] = rim

    edge = pltpu.VMEM((levels, cut + 16, LANES), jnp.bfloat16)
    return pl.pallas_call(
        body,
        out_shape=(edge, edge),
        scratch_shapes=[pltpu.VMEM((cut, LANES), jnp.float32), pltpu.VMEM((cut, LANES), jnp.float32)],
        name="edges_of",
    )(resident(main))


def weights_of(place, disp, total_rows):
    levels, rows = disp.shape[1:3]
    groups = rows // 8
    weight_count = 2 * SPAN + levels

    def body(place_ref, disp_ref, weight_ref):
        sub = iota2(0)
        anchor = place_ref[0]

        def weigh(k, carry):
            for g in range(groups):
                at = pl.ds(8 * g, 8)
                row_index = sub + (8 * g) + anchor
                zdep = jnp.clip(k.astype(jnp.float32) - disp_ref[0, k, at, :], 0.0, levels - 1.0)
                ydep = jnp.clip(row_index.astype(jnp.float32) - disp_ref[1, k, at, :], 0.0, total_rows - 1.0)
                xrel = -disp_ref[2, k, at, :]
                zb = jnp.floor(zdep)
                yb = jnp.floor(ydep)
                xb = jnp.floor(xrel)
                x_weights = spread(xb.astype(jnp.int32) - 1, cubic_weights(xrel - xb), -4, 4)
                y_weights = spread(yb.astype(jnp.int32) - row_index - 1, cubic_weights(ydep - yb), -4, 4)
                z_weights = spread(zb.astype(jnp.int32) - 1, cubic_weights(zdep - zb), 0, levels - 1)
                for n, value in enumerate(x_weights + y_weights + z_weights):
                    weight_ref[(k * groups + g) * weight_count + n] = value
            return carry

        lax.fori_loop(0, levels, weigh, 0)

    smem = pl.BlockSpec(memory_space=pltpu.SMEM)
    vmem = pl.BlockSpec(memory_space=pltpu.VMEM)
    return pl.pallas_call(
        body,
        out_shape=pltpu.VMEM((levels * groups * weight_count, 8, LANES), jnp.float32),
        in_specs=[smem, vmem],
        name="weights_of",
    )(place, disp)


def interpolate(place, weights, main, below, above, ntrac, rows, total_rows):
    levels = main.shape[0]
    height = ntrac * rows + 16
    groups = rows // 8
    tall = rows + 2 * RIM
    weight_count = 2 * SPAN + levels
    cut = ntrac * RIM

    def body(
        place_ref, weight_ref, main_ref, below_ref, above_ref, out_ref, rim_ref, end_ref, shifted_ref
    ):
        lane = iota2(1)
        sub = iota2(0)
        has_below = place_ref[0] > 0
        has_above = place_ref[0] + rows < total_rows

        for l in range(levels):
            rim_ref[l, 0] = main_ref[l, height - 16 : height, :].astype(jnp.float32)
            rim_ref[l, 1] = jnp.where(has_below, below_ref[l, cut:, :].astype(jnp.float32), 0.0)
            rim_ref[l, 2] = jnp.where(has_above, above_ref[l, cut:, :].astype(jnp.float32), 0.0)
            end_ref[l, 0] = jnp.where(has_below, below_ref[l, :cut, :].astype(jnp.float32), 0.0)
            end_ref[l, 1] = jnp.where(has_above, above_ref[l, :cut, :].astype(jnp.float32), 0.0)

        near = (lane + RIM) & 7

        def build(t):
            base = pl.multiple_of(t * rows, rows)
            for l in range(levels):
                own = jnp.broadcast_to(rim_ref[l, 0, pl.ds(t, 1), :], (8, LANES))
                block = main_ref[l, pl.ds(base, rows), :].astype(jnp.float32)
                ends = [end_ref[l, n, pl.ds(t * RIM, RIM), :] for n in range(2)]
                block = jnp.concatenate([ends[0], block, ends[1]], axis=0)
                lower = jnp.broadcast_to(rim_ref[l, 1, pl.ds(t, 1), :], (8, LANES))
                upper = jnp.broadcast_to(rim_ref[l, 2, pl.ds(t, 1), :], (8, LANES))
                for v in range(tall // 8):
                    inner_row = sub + (8 * v - RIM)
                    source = own
                    if v == 0:
                        source = jnp.where(sub < RIM, lower, own)
                    if v == tall // 8 - 1:
                        source = jnp.where(sub >= RIM, upper, own)
                    edges = lane_pick(source, ((inner_row & (rows - 1)) << 3) + near)
                    middle = block[8 * v : 8 * v + 8]
                    for ix in range(SPAN):
                        o = ix - RIM
                        if o > 0:
                            value = pltpu.roll(jnp.where(lane < o, edges, middle), LANES - o, 1)
                        elif o < 0:
                            value = pltpu.roll(jnp.where(lane >= LANES + o, edges, middle), -o, 1)
                        else:
                            value = middle
                        shifted_ref[l * SPAN + ix, 8 * v : 8 * v + 8, :] = value

        def cells(t, kp):
            results = [[], []]
            for g in range(groups):
                at = [((2 * kp + h) * groups + g) * weight_count for h in range(2)]
                wx = [[weight_ref[at[h] + n] for n in range(SPAN)] for h in range(2)]
                result = [None, None]
                for l in range(levels):
                    plane = [None, None]
                    for iy in range(SPAN):
                        line = [None, None]
                        first = 8 * g + iy
                        for ix in range(SPAN):
                            value = shifted_ref[l * SPAN + ix, first : first + 8, :]
                            for h in range(2):
                                term = wx[h][ix] * value
                                line[h] = term if ix == 0 else line[h] + term
                        for h in range(2):
                            term = weight_ref[at[h] + SPAN + iy] * line[h]
                            plane[h] = term if plane[h] is None else plane[h] + term
                    for h in range(2):
                        term = weight_ref[at[h] + 2 * SPAN + l] * plane[h]
                        result[h] = term if l == 0 else result[h] + term
                for h in range(2):
                    results[h].append(result[h])
            for h in range(2):
                out_ref[t, 2 * kp + h] = jnp.concatenate(results[h], axis=0).astype(jnp.bfloat16)

        def tracer(t, carry):
            build(t)

            def pairs(kp, inner):
                cells(t, kp)
                return inner

            lax.fori_loop(0, levels // 2, pairs, 0)
            return carry

        lax.fori_loop(0, ntrac, tracer, 0)

    smem = pl.BlockSpec(memory_space=pltpu.SMEM)
    vmem = pl.BlockSpec(memory_space=pltpu.VMEM)
    return pl.pallas_call(
        body,
        out_shape=jax.ShapeDtypeStruct((ntrac, levels, rows, LANES), jnp.bfloat16),
        in_specs=[smem] + [vmem] * 4,
        scratch_shapes=[
            pltpu.VMEM((levels, 3, 16, LANES), jnp.float32),
            pltpu.VMEM((levels, 2, cut, LANES), jnp.float32),
            pltpu.VMEM((levels * SPAN, tall, LANES), jnp.float32),
        ],
        name="interpolate",
    )(place, resident(weights), resident(main), resident(below), resident(above))


def parity_shift(x, by):
    tall = lax.axis_size("lat")
    wide = lax.axis_size("lon")
    pairs = []
    for a in range(tall):
        way = -by if a & 1 else by
        pairs += [(a * wide + b, a * wide + (b + way) % wide) for b in range(wide)]
    return lax.ppermute(x, ("lat", "lon"), pairs)


def local(tracers, winds, zonal_shift):
    ntrac, _, rows, _ = tracers.shape
    sectors = lax.axis_size("lon")
    total_rows = rows * lax.axis_size("lat")
    anchor = lax.axis_index("lat") * rows
    place = anchor.reshape(1)
    shifts = jnp.broadcast_to(zonal_shift[:, None], (rows, LANES))
    odd = lax.axis_index("lat") & 1
    main, hops = prepare(tracers, shifts, odd.reshape(1), sectors)
    top = sectors.bit_length() - 2
    for bit in [*range(top - 2), top, top - 1, top - 2]:
        moved = parity_shift(main, 1 << bit)
        main = jnp.where((hops >> bit & 1) == 1, moved, main)
    disp = trajectory(winds, anchor, total_rows)
    weights = weights_of(place, disp, total_rows)
    first, last = edges_of(main, ntrac, rows)
    below = ring_shift(last, "lat", 1)
    above = ring_shift(first, "lat", -1)
    new = interpolate(place, weights, main, below, above, ntrac, rows, total_rows)
    return new, disp


def solution(mesh):
    return jax.shard_map(
        local,
        mesh=mesh,
        in_specs=(P(None, None, "lat", "lon"), P(None, None, "lat", "lon"), P("lat")),
        out_specs=(P(None, None, "lat", "lon"), P(None, None, "lat", "lon")),
        check_vma=False,
    )
```
